32 devices in a mesh: prow: 4 (over y, core), pcol: 8 (over z, x).
Axes of the slice: x: 2, y: 2, z: 4, core: 2. Of those that a mesh axis runs over, the one named last changes fastest.
Arguments:
- matrix_slab: float32 [2048, 2048], P('pcol', 'prow'), may hold values from -1024 to 1024
- contributions: float32 [4, 256, 64, 256], P('prow', 'pcol'), may hold values from -3 to 3
- target_column: int32 [4, 256], P('prow', 'pcol'), may hold values from 0 to 31, as said below
- target_rows: int32 [4, 256], P('prow', 'pcol'), may hold values from 0 to 1
- live_rows: int32 [4, 256], P('prow', 'pcol'), may hold values from 1 to 256
- pivot_index: int32 [1, 256], replicated, may hold values from 256 to 2047, as said below
Outputs:
- factored: float32 [2048, 2048], P('pcol', 'prow')
The draws below stay inside these ranges and needn't reach their ends.
Inputs may be any that keep to these rules, and one draw needn't show every extreme that they name: `pivot_index`: row k lists 256 distinct rows, each (k + 1) * 256 or more. `target_column`: of the 32 blocks held by one device, at most 8 have target column blocks within the columns of one index of pcol, and exactly 8 for some index.
All inputs are finite; a program needn't handle non-finite values.
Results may differ from the reference program's by a relative error of at most 0.0001.
Values sent between devices are 32-bit elements; how exact they have to be, the bound alone decides.
A program may use at most 128 MiB of HBM per device.

```python
import jax
import jax.numpy as jnp
from jax import lax

SLAB = 2048
PW = 256
PANELS = 1
NB = 64
TR = 256
CB_DEV = 32
ROWS_DEV = 512
COLS_DEV = 256
ROWS = 2048
MOST = 8
CB_ALL = 256
N_PROW = 4
N_PCOL = 8


def pivot_draw(key):
    pivot_list = []
    for panel_number in range(PANELS):
        offset = (panel_number + 1) * PW
        shuffled = jax.random.permutation(jax.random.fold_in(key, panel_number), ROWS - offset)
        pivot_list.append(shuffled[:PW] + offset)
    return jnp.stack(pivot_list).astype(jnp.int32)


def draw_pivot_index(key, part):
    return pivot_draw(jax.random.fold_in(key, 11))


def draw_matrix_slab(key, part):
    pivots = pivot_draw(jax.random.fold_in(key, 11))
    subkeys = jax.random.split(jax.random.fold_in(key, 23), 6)
    modest = jax.random.uniform(subkeys[0], (SLAB, ROWS), jnp.float32, -1.0, 1.0)
    strong = jax.random.uniform(subkeys[1], (SLAB, ROWS), jnp.float32, -1.0, 1.0) * PW
    initial = jnp.arange(ROWS, dtype=jnp.int32)
    already_used = jnp.zeros((ROWS,), jnp.bool_)
    pivot_marks = []
    holders = []
    for panel_number in range(PANELS):
        chosen = pivots[panel_number]
        source_rows = initial[chosen]
        already_used = already_used.at[source_rows].set(True)
        pivot_marks.append(already_used)
        holders.append(source_rows)
        panel_slots = jnp.arange(panel_number * PW, (panel_number + 1) * PW, dtype=jnp.int32)
        moved_out = initial[panel_slots]
        initial = initial.at[panel_slots].set(source_rows).at[chosen].set(moved_out)
    pivot_marks = jnp.stack(pivot_marks)
    column_panel = jnp.minimum(jnp.arange(SLAB) // PW, PANELS - 1)
    in_panels = (jnp.arange(SLAB) < PANELS * PW)[:, None]
    quiet_mask = jnp.logical_or(jnp.logical_not(in_panels), pivot_marks[column_panel])
    entries = jnp.where(quiet_mask, modest, strong)
    for panel_number in range(PANELS):
        panel_columns = panel_number * PW + jnp.arange(PW)
        block_entries = jax.random.uniform(jax.random.fold_in(subkeys[5], panel_number), (PW, PW), jnp.float32, -0.25 * PW, 0.25 * PW)
        entries = entries.at[panel_columns[:, None], holders[panel_number][None, :]].set(block_entries)
        sign_flip = jnp.where(jax.random.bernoulli(jax.random.fold_in(subkeys[2], panel_number), 0.5, (PW,)), 1.0, -1.0)
        magnitude = jax.random.uniform(jax.random.fold_in(subkeys[3], panel_number), (PW,), jnp.float32, 3.0 * PW, 4.0 * PW)
        entries = entries.at[panel_columns, holders[panel_number]].set(sign_flip * magnitude)
    return entries


def draw_target_column(key, part):
    local_blocks = COLS_DEV // NB

    def one_device(device_key):
        first_key, second_key, third_key, fourth_key = jax.random.split(device_key, 4)
        slot_owner = jnp.arange(N_PCOL * MOST, dtype=jnp.int32) // MOST
        busiest = jax.random.randint(first_key, (), 0, N_PCOL)
        others = jax.random.permutation(second_key, N_PCOL * MOST - MOST)[:CB_DEV - MOST] + MOST
        picked = jnp.concatenate([jnp.arange(MOST, dtype=jnp.int32), others.astype(jnp.int32)])
        owners = (slot_owner[picked] + busiest) % N_PCOL
        owners = owners[jax.random.permutation(third_key, CB_DEV)]
        within = jax.random.randint(fourth_key, (CB_DEV,), 0, local_blocks)
        return owners * local_blocks + within
    device_keys = jax.random.split(jax.random.fold_in(key, 31), N_PROW * N_PCOL)
    return jax.vmap(one_device)(device_keys).reshape(N_PROW, N_PCOL * CB_DEV).astype(jnp.int32)


def set_ends(values, own_key, low, high):
    longest = values.shape.index(max(values.shape))
    spots = []
    for shift in (0, 1):
        where = [jax.random.randint(jax.random.fold_in(own_key, axis), (), 0, length) for axis, length in enumerate(values.shape)]
        where[longest] = (where[longest] + shift) % values.shape[longest]
        spots.append(tuple(where))
    return values.at[spots[0]].set(low).at[spots[1]].set(high)


def shard_levels(key, shape, shards, low, largest):
    def one(dim, blocks):
        draws = jax.random.uniform(jax.random.fold_in(jax.random.fold_in(key, 6), dim), (blocks,), jnp.float32, low / len(shards), largest / len(shards))
        return jnp.repeat(jnp.exp(draws), shape[dim] // blocks).reshape((-1,) + (1,) * (len(shape) - dim - 1))

    level = one(*shards[0])
    for cut in shards[1:]:
        level = level * one(*cut)
    return level


def scatter_about(own_key, shape, scale, limit, cuts=(), kind=jnp.bfloat16):
    level = shard_levels(own_key, shape, cuts, -0.22, 0.18) if cuts else 1.0
    values = jax.random.normal(own_key, shape, jnp.float32) * scale * level
    return jnp.minimum(jnp.maximum(values, -limit), limit).astype(kind)


def setup_inputs(seed: int = 0) -> dict:
    keys = jax.random.split(jax.random.key(seed), 7)
    return {
        "matrix_slab": draw_matrix_slab(jax.random.fold_in(keys[6], 71), 0),
        "contributions": scatter_about(keys[1], (N_PROW, CB_ALL, NB, TR), 0.5, 3.0, ((0, 4), (1, 8)), jnp.float32),
        "target_column": draw_target_column(jax.random.fold_in(keys[6], 71), 0),
        "target_rows": set_ends(jax.random.randint(keys[3], (N_PROW, CB_ALL), 0, ROWS_DEV // TR), jax.random.fold_in(keys[3], 1), 0, (ROWS_DEV // TR) - 1).astype(jnp.int32),
        "live_rows": set_ends(jax.random.randint(keys[4], (N_PROW, CB_ALL), 1, TR + 1), jax.random.fold_in(keys[4], 1), 1, TR).astype(jnp.int32),
        "pivot_index": draw_pivot_index(jax.random.fold_in(keys[6], 71), 0),
    }


HIGHEST = lax.Precision.HIGHEST

def factor_block(square):
    extent = square.shape[0]
    if extent <= 16:
        for column in range(extent - 1):
            ratios = square[column + 1:, column] / square[column, column]
            square = square.at[column + 1:, column].set(ratios)
            square = square.at[column + 1:, column + 1:].add(-ratios[:, None] * square[column, column + 1:][None, :])
        return square
    middle = extent // 2
    top_left = factor_block(square[:middle, :middle])
    lower_unit = jnp.tril(top_left, -1) + jnp.eye(middle, dtype=square.dtype)
    upper_part = jnp.triu(top_left)
    right_part = jax.scipy.linalg.solve_triangular(lower_unit, square[:middle, middle:], lower=True, unit_diagonal=True)
    left_part = jax.scipy.linalg.solve_triangular(upper_part.T, square[middle:, :middle].T, lower=True).T
    schur_part = square[middle:, middle:] - jnp.dot(left_part, right_part, precision=HIGHEST)
    bottom = factor_block(schur_part)
    upper_half = jnp.concatenate([top_left, right_part], axis=1)
    lower_half = jnp.concatenate([left_part, bottom], axis=1)
    return jnp.concatenate([upper_half, lower_half], axis=0)

def split_factors(packed):
    extent = packed.shape[0]
    lower_unit = jnp.tril(packed, -1) + jnp.eye(extent, dtype=packed.dtype)
    return (lower_unit, jnp.triu(packed))

def reference(matrix_slab, contributions, target_column, target_rows, live_rows, pivot_index):
    blocks = contributions.reshape(N_PROW * CB_ALL, NB, TR)
    lengths = live_rows.reshape(-1)
    column_anchor = (target_column.reshape(-1) * NB).astype(jnp.int32)
    row_anchor = (jnp.arange(N_PROW, dtype=jnp.int32)[:, None] * ROWS_DEV + target_rows * TR).reshape(-1).astype(jnp.int32)
    positions = jnp.arange(TR, dtype=jnp.int32)

    def add_block(index, current):
        single = blocks[index] * (positions < lengths[index]).astype(blocks.dtype)[None, :]
        anchor = (column_anchor[index], row_anchor[index])
        window = lax.dynamic_slice(current, anchor, (NB, TR))
        return lax.dynamic_update_slice(current, window + single, anchor)
    matrix = lax.fori_loop(0, N_PROW * CB_ALL, add_block, matrix_slab)
    rows_all = jnp.arange(ROWS, dtype=jnp.int32)
    for panel_number in range(PANELS):
        panel_start = panel_number * PW
        panel_end = panel_start + PW
        chosen = pivot_index[panel_number]
        displaced = matrix[:, panel_start:panel_end]
        incoming = matrix[:, chosen]
        matrix = matrix.at[:, chosen].set(displaced)
        matrix = matrix.at[:, panel_start:panel_end].set(incoming)
        panel_cols = matrix[panel_start:panel_end, :]
        packed = factor_block(panel_cols[:, panel_start:panel_end].T)
        lower_unit, upper_part = split_factors(packed)
        lower_cols = jax.scipy.linalg.solve_triangular(upper_part.T, panel_cols, lower=True)
        upper_rows = jax.scipy.linalg.solve_triangular(lower_unit, matrix[:, panel_start:panel_end].T, lower=True, unit_diagonal=True)
        below_rows = rows_all >= panel_end
        renewed = panel_cols.at[:, panel_start:panel_end].set(packed.T)
        renewed = jnp.where(below_rows[None, :], lower_cols, renewed)
        trailing = upper_rows[:, panel_end:].T
        update = jnp.dot(trailing, lower_cols[:, panel_end:], precision=HIGHEST)
        matrix = matrix.at[panel_start:panel_end, :].set(renewed)
        matrix = matrix.at[panel_end:, panel_start:panel_end].set(trailing)
        matrix = matrix.at[panel_end:, panel_end:].add(-update)
    return matrix
```

```python
import functools

import jax
import jax.numpy as jnp
from jax import lax
from jax.experimental import pallas as pl
from jax.experimental.pallas import tpu as pltpu
from jax.sharding import PartitionSpec as P

PW = 256
NB = 64
TR = 256
B = 64

HIGHEST = lax.Precision.HIGHEST
VMEM = pltpu.VMEM
F32 = jnp.float32


def hdot(a, b):
    return jnp.dot(a, b, precision=HIGHEST, preferred_element_type=F32)


def spread_kernel(tc, tr, lr, place, pivots, blocks, slab, dense, diag, lead):
    cols = slab.shape[0]
    rows = slab.shape[1]
    dense[...] = jnp.zeros_like(dense)
    own = pl.multiple_of(place[1] * cols, cols)
    dense[pl.ds(own, cols), :] = slab[...]
    lane = lax.broadcasted_iota(jnp.int32, (NB, TR), 1)

    def add(index, carry):
        c = pl.multiple_of(tc[index] * NB, NB)
        r = pl.multiple_of(tr[index] * TR, TR)
        block = jnp.where(lane < lr[index], blocks[index], 0.0)
        dense[pl.ds(c, NB), pl.ds(r, TR)] += block
        return carry

    lax.fori_loop(0, blocks.shape[0], add, 0)
    row = place[0] * rows + lax.broadcasted_iota(jnp.int32, (PW, rows), 1)
    pick = (pivots[...] == row).astype(F32)
    panel = dense[0:PW, :]
    diag[...] = lax.dot_general(
        panel, pick, (((1,), (1,)), ((), ())), precision=HIGHEST, preferred_element_type=F32
    )
    lead[...] = jnp.where(place[0] == 0, panel[:, 0:PW], 0.0)


def eliminate(a):
    groups = B // 8
    eye = (
        lax.broadcasted_iota(jnp.int32, (B, B), 0) == lax.broadcasted_iota(jnp.int32, (B, B), 1)
    ).astype(F32)
    first = jnp.concatenate([a, eye], axis=1)
    second = jnp.concatenate([a.T, eye], axis=1)
    one = [first[8 * g : 8 * g + 8] for g in range(groups)]
    two = [second[8 * g : 8 * g + 8] for g in range(groups)]
    sub = lax.broadcasted_iota(jnp.int32, (8, 2 * B), 0)
    for k in range(B):
        g0, s0 = divmod(k, 8)
        below = sub > s0
        for which, held in enumerate((one, two)):
            col = jnp.broadcast_to(held[g0][:, k : k + 1], (8, 2 * B))
            scaled = jnp.broadcast_to((held[g0] / col)[s0 : s0 + 1, :], (8, 2 * B))
            for g in range(g0 + 1, groups):
                held[g] = held[g] - held[g][:, k : k + 1] * scaled
            fresh = held[g0] - jnp.where(below, col, 0.0) * scaled
            held[g0] = jnp.where(sub == s0, scaled, fresh) if which == 0 else fresh
    first = jnp.concatenate(one, axis=0)
    second = jnp.concatenate(two, axis=0)
    return second[:, :B].T, first[:, :B], first[:, B:], second[:, B:].T


def factor_kernel(source, packed, low_inv, up_inv):
    packed[...] = source[...]
    i = lax.broadcasted_iota(jnp.int32, (B, B), 0)
    j = lax.broadcasted_iota(jnp.int32, (B, B), 1)
    for s in range(0, PW, B):
        e = s + B
        low, up, li, ui = eliminate(packed[s:e, s:e])
        li = jnp.where(i >= j, li, 0.0)
        ui = jnp.where(i <= j, ui, 0.0)
        packed[s:e, s:e] = jnp.where(i >= j, low, up)
        low_inv[s:e, :] = li
        up_inv[s:e, :] = ui
        if e < PW:
            right = hdot(li, packed[s:e, e:])
            left = hdot(packed[e:, s:e], ui)
            packed[s:e, e:] = right
            packed[e:, s:e] = left
            packed[e:, e:] = packed[e:, e:] - hdot(left, right)


def finish_kernel(
    place, pivots, packed, low_inv, up_inv, panel, lead, diag, matrix, incoming, moved, out, x, y
):
    cols, rows = matrix.shape
    row = place[0] * rows + lax.broadcasted_iota(jnp.int32, (PW, rows), 1)
    pick = (pivots[...] == row).astype(F32)
    hit = jnp.sum(pick, axis=0, keepdims=True) > 0.0
    head = place[0] == 0
    x[...] = jnp.where(hit, hdot(lead[...], pick), panel[...])
    x[:, 0:PW] = jnp.where(head, diag[...], x[:, 0:PW])
    for s in range(0, PW, B):
        e = s + B
        part = x[s:e, :]
        if s:
            part = part - hdot(packed[s:e, 0:s], x[0:s, :])
        x[s:e, :] = hdot(low_inv[s:e, :], part)
        part = incoming[:, s:e]
        if s:
            part = part - hdot(y[:, 0:s], packed[0:s, s:e])
        y[:, s:e] = hdot(part, up_inv[s:e, :])
    owners = PW // cols

    @pl.when(place[1] >= owners)
    def _():
        swapped = jnp.where(hit, hdot(moved[...], pick), matrix[...])
        out[...] = swapped - hdot(y[...], x[...])
        out[:, 0:PW] = jnp.where(head, y[...], out[:, 0:PW])

    @pl.when(place[1] < owners)
    def _():
        x[:, 0:PW] = jnp.where(head, packed[...], x[:, 0:PW])
        off = pl.multiple_of(lax.rem(place[1], owners) * cols, cols)
        out[...] = x[pl.ds(off, cols), :]


def shape(*dims):
    return jax.ShapeDtypeStruct(dims, F32)


SMEM_SPEC = pl.BlockSpec(memory_space=pltpu.SMEM)
VMEM_SPEC = pl.BlockSpec(memory_space=pltpu.VMEM)
PARAMS = pltpu.CompilerParams(vmem_limit_bytes=48 * 1024 * 1024)


def per_device(slab_cols, matrix_slab, contributions, target_column, target_rows, live_rows, pivot_index):
    cols, rows = matrix_slab.shape
    row_group = lax.axis_index("prow")
    col_group = lax.axis_index("pcol")
    place = jnp.stack([row_group, col_group]).astype(jnp.int32)
    pivots = pivot_index[0][:, None]
    dense, diag_part, lead_part = pl.pallas_call(
        spread_kernel,
        out_shape=(shape(slab_cols, rows), shape(PW, PW), shape(PW, PW)),
        in_specs=[SMEM_SPEC] * 4 + [VMEM_SPEC] * 3,
        out_specs=(VMEM_SPEC,) * 3,
        compiler_params=PARAMS,
    )(target_column[0], target_rows[0], live_rows[0], place, pivots, contributions[0], matrix_slab)
    diag = lax.psum(diag_part, ("prow", "pcol"))
    packed, low_inv, up_inv = pl.pallas_call(
        factor_kernel,
        out_shape=(shape(PW, PW), shape(PW, B), shape(PW, B)),
        in_specs=[VMEM_SPEC],
        out_specs=(VMEM_SPEC,) * 3,
        compiler_params=PARAMS,
        cost_estimate=pl.CostEstimate(flops=10**10, bytes_accessed=10**7, transcendentals=0),
    )(diag)
    matrix = lax.psum_scatter(dense, "pcol", scatter_dimension=0, tiled=True)
    panel = lax.psum(dense[0:PW], "pcol")
    lead = lax.psum(lead_part, ("prow", "pcol"))
    global_rows = row_group * rows + jnp.arange(rows)
    pick = (pivots == global_rows[None, :]).astype(F32)
    mine = jnp.concatenate(
        [
            jnp.dot(matrix, pick.T, precision=HIGHEST),
            jnp.where(row_group == 0, matrix[:, 0:PW], 0.0),
        ],
        axis=0,
    )
    both = lax.psum(mine, "prow")
    return pl.pallas_call(
        finish_kernel,
        out_shape=shape(cols, rows),
        in_specs=[SMEM_SPEC] + [VMEM_SPEC] * 10,
        out_specs=VMEM_SPEC,
        scratch_shapes=[VMEM((PW, rows), F32), VMEM((cols, PW), F32)],
        compiler_params=PARAMS,
    )(place, pivots, packed, low_inv, up_inv, panel, lead, diag, matrix, both[:cols], both[cols:])


def solution(mesh):
    placed = (
        P("pcol", "prow"),
        P("prow", "pcol", None, None),
        P("prow", "pcol"),
        P("prow", "pcol"),
        P("prow", "pcol"),
        P(),
    )

    def whole(matrix_slab, *rest):
        return jax.shard_map(
            functools.partial(per_device, matrix_slab.shape[0]),
            mesh=mesh,
            in_specs=placed,
            out_specs=P("pcol", "prow"),
            check_vma=False,
        )(matrix_slab, *rest)

    return whole
```

```python
import functools

import jax
import jax.numpy as jnp
from jax import lax
from jax.experimental import pallas as pl
from jax.experimental.pallas import tpu as pltpu
from jax.sharding import PartitionSpec as P

PW = 256
NB = 64
TR = 256
B = 64

HIGHEST = lax.Precision.HIGHEST
VMEM = pltpu.VMEM
F32 = jnp.float32


def hdot(a, b):
    return jnp.dot(a, b, precision=HIGHEST, preferred_element_type=F32)


def spread_kernel(tc, tr, lr, place, blocks, slab, dense):
    cols = slab.shape[0]
    dense[...] = jnp.zeros_like(dense)
    own = pl.multiple_of(place[1] * cols, cols)
    dense[pl.ds(own, cols), :] = slab[...]
    lane = lax.broadcasted_iota(jnp.int32, (NB, TR), 1)

    def add(index, carry):
        c = pl.multiple_of(tc[index] * NB, NB)
        r = pl.multiple_of(tr[index] * TR, TR)
        block = jnp.where(lane < lr[index], blocks[index], 0.0)
        dense[pl.ds(c, NB), pl.ds(r, TR)] += block
        return carry

    lax.fori_loop(0, blocks.shape[0], add, 0)


def eliminate(a):
    groups = B // 8
    eye = (
        lax.broadcasted_iota(jnp.int32, (B, B), 0) == lax.broadcasted_iota(jnp.int32, (B, B), 1)
    ).astype(F32)
    first = jnp.concatenate([a, eye], axis=1)
    second = jnp.concatenate([a.T, eye], axis=1)
    one = [first[8 * g : 8 * g + 8] for g in range(groups)]
    two = [second[8 * g : 8 * g + 8] for g in range(groups)]
    sub = lax.broadcasted_iota(jnp.int32, (8, 2 * B), 0)
    for k in range(B):
        g0, s0 = divmod(k, 8)
        below = sub > s0
        for which, held in enumerate((one, two)):
            col = jnp.broadcast_to(held[g0][:, k : k + 1], (8, 2 * B))
            scaled = jnp.broadcast_to((held[g0] / col)[s0 : s0 + 1, :], (8, 2 * B))
            for g in range(g0 + 1, groups):
                held[g] = held[g] - held[g][:, k : k + 1] * scaled
            fresh = held[g0] - jnp.where(below, col, 0.0) * scaled
            held[g0] = jnp.where(sub == s0, scaled, fresh) if which == 0 else fresh
    first = jnp.concatenate(one, axis=0)
    second = jnp.concatenate(two, axis=0)
    return second[:, :B].T, first[:, :B], first[:, B:], second[:, B:].T


def factor_kernel(source, packed, low_inv, up_inv):
    packed[...] = source[...]
    i = lax.broadcasted_iota(jnp.int32, (B, B), 0)
    j = lax.broadcasted_iota(jnp.int32, (B, B), 1)
    for s in range(0, PW, B):
        e = s + B
        low, up, li, ui = eliminate(packed[s:e, s:e])
        li = jnp.where(i >= j, li, 0.0)
        ui = jnp.where(i <= j, ui, 0.0)
        packed[s:e, s:e] = jnp.where(i >= j, low, up)
        low_inv[s:e, :] = li
        up_inv[s:e, :] = ui
        if e < PW:
            right = hdot(li, packed[s:e, e:])
            left = hdot(packed[e:, s:e], ui)
            packed[s:e, e:] = right
            packed[e:, s:e] = left
            packed[e:, e:] = packed[e:, e:] - hdot(left, right)


def finish_kernel(
    place, pivots, packed, low_inv, up_inv, panel, lead, diag, matrix, incoming, moved, out, x, y
):
    cols, rows = matrix.shape
    row = place[0] * rows + lax.broadcasted_iota(jnp.int32, (PW, rows), 1)
    pick = (pivots[...] == row).astype(F32)
    hit = jnp.sum(pick, axis=0, keepdims=True) > 0.0
    head = place[0] == 0
    x[...] = jnp.where(hit, hdot(lead[...], pick), panel[...])
    x[:, 0:PW] = jnp.where(head, diag[...], x[:, 0:PW])
    for s in range(0, PW, B):
        e = s + B
        part = x[s:e, :]
        if s:
            part = part - hdot(packed[s:e, 0:s], x[0:s, :])
        x[s:e, :] = hdot(low_inv[s:e, :], part)
        part = incoming[:, s:e]
        if s:
            part = part - hdot(y[:, 0:s], packed[0:s, s:e])
        y[:, s:e] = hdot(part, up_inv[s:e, :])
    owners = PW // cols

    @pl.when(place[1] >= owners)
    def _():
        swapped = jnp.where(hit, hdot(moved[...], pick), matrix[...])
        out[...] = swapped - hdot(y[...], x[...])
        out[:, 0:PW] = jnp.where(head, y[...], out[:, 0:PW])

    @pl.when(place[1] < owners)
    def _():
        x[:, 0:PW] = jnp.where(head, packed[...], x[:, 0:PW])
        off = pl.multiple_of(lax.rem(place[1], owners) * cols, cols)
        out[...] = x[pl.ds(off, cols), :]


def shape(*dims):
    return jax.ShapeDtypeStruct(dims, F32)


SMEM_SPEC = pl.BlockSpec(memory_space=pltpu.SMEM)
VMEM_SPEC = pl.BlockSpec(memory_space=pltpu.VMEM)
PARAMS = pltpu.CompilerParams(vmem_limit_bytes=48 * 1024 * 1024)


def per_device(slab_cols, matrix_slab, contributions, target_column, target_rows, live_rows, pivot_index):
    cols, rows = matrix_slab.shape
    row_group = lax.axis_index("prow")
    col_group = lax.axis_index("pcol")
    place = jnp.stack([row_group, col_group]).astype(jnp.int32)
    pivots = pivot_index[0][:, None]
    dense = pl.pallas_call(
        spread_kernel,
        out_shape=shape(slab_cols, rows),
        in_specs=[SMEM_SPEC] * 4 + [VMEM_SPEC] * 2,
        out_specs=VMEM_SPEC,
        compiler_params=PARAMS,
    )(target_column[0], target_rows[0], live_rows[0], place, contributions[0], matrix_slab)
    piece = lax.psum_scatter(dense[0:PW], "pcol", scatter_dimension=0, tiled=True)
    panel = lax.all_gather(piece, "pcol", axis=0, tiled=True)
    global_rows = row_group * rows + jnp.arange(rows)
    pick = (pivots == global_rows[None, :]).astype(F32)
    leading = jnp.concatenate(
        [
            jnp.dot(panel, pick.T, precision=HIGHEST),
            jnp.where(row_group == 0, panel[:, 0:PW], 0.0),
        ],
        axis=0,
    )
    leading = lax.psum(leading, "prow")
    diag, lead = leading[:PW], leading[PW:]
    packed, low_inv, up_inv = pl.pallas_call(
        factor_kernel,
        out_shape=(shape(PW, PW), shape(PW, B), shape(PW, B)),
        in_specs=[VMEM_SPEC],
        out_specs=(VMEM_SPEC,) * 3,
        compiler_params=PARAMS,
        cost_estimate=pl.CostEstimate(flops=10**10, bytes_accessed=10**7, transcendentals=0),
    )(diag)
    matrix = lax.psum_scatter(dense, "pcol", scatter_dimension=0, tiled=True)
    mine = jnp.concatenate(
        [
            jnp.dot(matrix, pick.T, precision=HIGHEST),
            jnp.where(row_group == 0, matrix[:, 0:PW], 0.0),
        ],
        axis=0,
    )
    both = lax.psum(mine, "prow")
    return pl.pallas_call(
        finish_kernel,
        out_shape=shape(cols, rows),
        in_specs=[SMEM_SPEC] + [VMEM_SPEC] * 10,
        out_specs=VMEM_SPEC,
        scratch_shapes=[VMEM((PW, rows), F32), VMEM((cols, PW), F32)],
        compiler_params=PARAMS,
    )(place, pivots, packed, low_inv, up_inv, panel, lead, diag, matrix, both[:cols], both[cols:])


def solution(mesh):
    placed = (
        P("pcol", "prow"),
        P("prow", "pcol", None, None),
        P("prow", "pcol"),
        P("prow", "pcol"),
        P("prow", "pcol"),
        P(),
    )

    def whole(matrix_slab, *rest):
        return jax.shard_map(
            functools.partial(per_device, matrix_slab.shape[0]),
            mesh=mesh,
            in_specs=placed,
            out_specs=P("pcol", "prow"),
            check_vma=False,
        )(matrix_slab, *rest)

    return whole
```
